32 devices in a mesh: mod: 2 (over y), exp: 16 (over z, x, core).
Axes of the slice: x: 2, y: 2, z: 4, core: 2. Of those that a mesh axis runs over, the one named last changes fastest.
Arguments:
- tokens: bfloat16 [2, 8192, 1024], P('mod', 'exp'), may hold values from -60 to 60
- bottleneck: bfloat16 [64, 4, 1024], P('exp'), may hold values from -6 to 6
- clip_ids: int32 [2, 8192], P('mod', 'exp'), may hold values from 0 to 63, as said below
- expert_ids: int32 [2, 8192], P('mod', 'exp'), may hold values from 0 to 15, as said below
- slots: int32 [2, 8192], P('mod', 'exp'), may hold values from 0 to 127, as said below
- norm1_gain: bfloat16 [2, 1024], P('mod'), may hold values from 0.099609375 to 1.8984375
- attn_qkv: bfloat16 [2, 1024, 3072], P('mod'), may hold values from -2 to 2
- attn_out: bfloat16 [2, 1024, 1024], P('mod'), may hold values from -0.1875 to 0.1875
- norm2_gain: bfloat16 [2, 1024], P('mod'), may hold values from 0.099609375 to 1.8984375
- router: bfloat16 [1024, 16], replicated, may hold values from -0.1875 to 0.1875
- fc_in: bfloat16 [16, 1024, 4096], P('exp'), may hold values from -0.1875 to 0.1875
- fc_out: bfloat16 [16, 4096, 1024], P('exp'), may hold values from -0.09375 to 0.09375
Outputs:
- mixed_tokens: bfloat16 [2, 8192, 1024], P('mod', 'exp')
- new_bottleneck: bfloat16 [64, 4, 1024], P('exp')
The draws below stay inside these ranges and needn't reach their ends.
Inputs may be any that keep to these rules, and one draw needn't show every extreme that they name: `clip_ids`: Non-decreasing in each modality; the tokens of block b of 512 rows belong to clips b * 4 to (b + 1) * 4 - 1, each of which has one or more of them. `expert_ids`: each token's single expert. For the k tokens of one block of 512 rows of one modality that share an expert, the slots are 0 to k - 1 in some order; k is at most 128; in every block of each modality one expert, the same for all blocks of that modality, has k = 128.
All inputs are finite; a program needn't handle non-finite values.
Results may differ from the reference program's by a relative error of at most 0.0085.
Values may be sent and summed in bfloat16 or wider, within the bound.
A program may use at most 128 MiB of HBM per device.

```python
import math
import jax
import jax.numpy as jnp
from jax import lax

D = 1024
FF = 4096
HEAD = 64
NB = 4
TOK_DEV = 512
CLIPS_DEV = 4
EXPERTS = 16
TOKENS = 8192
CLIPS = 64
CAP = 64


def routing_table(key):
    blocks = TOKENS // TOK_DEV
    queue_len = 2 * CAP
    seat_count = EXPERTS * queue_len
    routing_key = jax.random.fold_in(key, 7001)
    hot_key, level_key, block_key = jax.random.split(routing_key, 3)
    hottest = jax.random.randint(hot_key, (2,), 0, EXPERTS)
    levels = jax.random.randint(level_key, (2, EXPERTS), 0, 4)
    block_seeds = jax.random.split(block_key, 2 * blocks)
    modality_of = jnp.arange(2 * blocks, dtype=jnp.int32) // blocks
    seat_index = jnp.arange(seat_count, dtype=jnp.int32)
    seat_expert = seat_index // queue_len

    def one_block(block_seed, modality):
        second_key, noise_key, order_key = jax.random.split(block_seed, 3)
        second = jax.random.randint(second_key, (), 0, EXPERTS)
        jitter = jax.random.randint(noise_key, (seat_count,), 0, 4096)
        favoured = (seat_expert == hottest[modality]) | (seat_expert == second)
        seat_score = jitter + levels[modality][seat_expert] * 1024 + jnp.where(favoured, 16384, 0)
        ranked = seat_score * seat_count + seat_index
        picked = lax.top_k(ranked, TOK_DEV)[1]
        marked = jnp.zeros((seat_count,), jnp.int32).at[picked].set(1)
        grouped = marked.reshape(EXPERTS, queue_len)
        rank_table = (jnp.cumsum(grouped, axis=1) - grouped).reshape(seat_count)
        token_order = jax.random.permutation(order_key, TOK_DEV)
        assigned = picked[token_order]
        return (seat_expert[assigned], rank_table[assigned])
    experts_drawn, slots_drawn = jax.vmap(one_block)(block_seeds, modality_of)
    return (experts_drawn.reshape(2, TOKENS).astype(jnp.int32), slots_drawn.reshape(2, TOKENS).astype(jnp.int32))


def draw_expert_ids(key, part):
    return routing_table(key)[0]


def draw_slots(key, part):
    return routing_table(key)[1]


def draw_clip_ids(key, part):
    blocks = TOKENS // TOK_DEV
    block_seeds = jax.random.split(jax.random.fold_in(key, 7002), 2 * blocks)
    position = jnp.arange(TOK_DEV, dtype=jnp.int32)

    def one_block(block_seed):
        cuts = jax.random.permutation(block_seed, TOK_DEV - 1)[:CLIPS_DEV - 1] + 1
        return jnp.sum((position[:, None] >= cuts[None, :]).astype(jnp.int32), axis=1)
    local_ids = jax.vmap(one_block)(block_seeds).reshape(2, blocks, TOK_DEV)
    offsets = jnp.arange(blocks, dtype=jnp.int32)[None, :, None] * CLIPS_DEV
    return (local_ids + offsets).reshape(2, TOKENS).astype(jnp.int32)


def draw_tokens(key, part):
    normal_draw = jnp.clip(jax.random.normal(key, (2, TOKENS, D), jnp.float32), -6.0, 6.0)
    return normal_draw.astype(jnp.bfloat16)


def draw_attn_qkv(key, part):
    unit_scale = 1.0 / math.sqrt(D)
    entries = jax.random.normal(key, (2, D, 3 * D), jnp.float32) * unit_scale
    return jnp.clip(entries, -2.0, 2.0).astype(jnp.bfloat16)


def shard_levels(stream_key, shape, pieces, smallest, top_value):
    gain = 1.0
    for dim, parts in pieces:
        steps = jax.random.uniform(jax.random.fold_in(jax.random.fold_in(stream_key, 6), dim), (parts,), jnp.float32, smallest / len(pieces), top_value / len(pieces))
        gain = gain * jnp.repeat(jnp.exp(steps), shape[dim] // parts).reshape((-1,) + (1,) * (len(shape) - 1 - dim))
    return gain


def scatter_about(stream_key, shape, scale, limit, cuts=(), kind=jnp.bfloat16):
    factor_of = shard_levels(stream_key, shape, cuts, -0.22, 0.18) if cuts else 1.0
    values = jax.random.normal(stream_key, shape, jnp.float32) * scale * factor_of
    return jnp.minimum(jnp.maximum(values, -limit), limit).astype(kind)


def setup_inputs(seed: int = 0) -> dict:
    key_list = jax.random.split(jax.random.key(seed), 13)
    return {
        "tokens": draw_tokens(jax.random.fold_in(key_list[12], 71), 0),
        "bottleneck": scatter_about(key_list[1], (CLIPS, NB, D), 1.0, 6.0, ((0, 16),)),
        "clip_ids": draw_clip_ids(jax.random.fold_in(key_list[12], 71), 0),
        "expert_ids": draw_expert_ids(jax.random.fold_in(key_list[12], 71), 0),
        "slots": draw_slots(jax.random.fold_in(key_list[12], 71), 0),
        "norm1_gain": jnp.clip(1.0 + 0.18 * jax.random.normal(key_list[5], (2, D), jnp.float32), 0.099609375, 1.8984375).astype(jnp.bfloat16),
        "attn_qkv": draw_attn_qkv(jax.random.fold_in(key_list[12], 71), 0),
        "attn_out": scatter_about(key_list[7], (2, D, D), D ** -0.5, 0.1875, ((0, 2),)),
        "norm2_gain": jnp.clip(1.0 + 0.18 * jax.random.normal(key_list[8], (2, D), jnp.float32), 0.099609375, 1.8984375).astype(jnp.bfloat16),
        "router": scatter_about(key_list[9], (D, EXPERTS), D ** -0.5, 0.1875),
        "fc_in": scatter_about(key_list[10], (EXPERTS, D, FF), D ** -0.5, 0.1875, ((0, 16),)),
        "fc_out": scatter_about(key_list[11], (EXPERTS, FF, D), FF ** -0.5, 0.09375, ((0, 16),)),
    }


EPSILON = 1e-06

def layer_norm(features, scales):
    row_mean = lax.optimization_barrier(jnp.mean(features, axis=-1, keepdims=True))
    centred = features - row_mean
    spread = lax.optimization_barrier(jnp.mean(centred * centred, axis=-1, keepdims=True))
    return centred * lax.rsqrt(spread + EPSILON) * scales.astype(jnp.float32)

def attend(token_rows, latent_rows, token_clip, clip_start, scales, w_qkv, w_out):
    n_clips, n_latent, model_width = latent_rows.shape
    n_tokens = token_rows.shape[0]
    all_rows = jnp.concatenate([token_rows, latent_rows.reshape(n_clips * n_latent, model_width)], axis=0)
    row_count = all_rows.shape[0]
    head_count = model_width // HEAD
    normed = layer_norm(all_rows.astype(jnp.float32), scales).astype(jnp.bfloat16)
    packed = jnp.dot(normed, w_qkv, preferred_element_type=jnp.float32).astype(jnp.bfloat16)
    queries = packed[:, :model_width].reshape(row_count, head_count, HEAD)
    key_rows = packed[:, model_width:2 * model_width].reshape(row_count, head_count, HEAD)
    value_rows = packed[:, 2 * model_width:].reshape(row_count, head_count, HEAD)
    latent_clip = clip_start + jnp.arange(n_clips * n_latent, dtype=jnp.int32) // n_latent
    row_clip = jnp.concatenate([token_clip.astype(jnp.int32), latent_clip.astype(jnp.int32)])
    allowed = row_clip[:, None] == row_clip[None, :]
    scores = jnp.einsum('qhd,khd->hqk', queries.astype(jnp.float32), key_rows.astype(jnp.float32)) * (1.0 / math.sqrt(HEAD))
    scores = jnp.where(allowed[None, :, :], scores, -jnp.inf)
    row_max = lax.optimization_barrier(jnp.max(scores, axis=-1, keepdims=True))
    weights = jnp.exp(scores - row_max)
    attn_weights = (weights / lax.optimization_barrier(jnp.sum(weights, axis=-1, keepdims=True))).astype(jnp.bfloat16)
    attended = jnp.einsum('hqk,khd->qhd', attn_weights.astype(jnp.float32), value_rows.astype(jnp.float32))
    attended = attended.reshape(row_count, model_width).astype(jnp.bfloat16)
    updated = all_rows.astype(jnp.float32) + jnp.dot(attended, w_out, preferred_element_type=jnp.float32)
    return (updated[:n_tokens], updated[n_tokens:].reshape(n_clips, n_latent, model_width))

def expert_step(operands):
    block_rows, weight_in, weight_out = operands
    hidden_units = jnp.dot(block_rows, weight_in, preferred_element_type=jnp.float32)
    activated = jax.nn.gelu(hidden_units, approximate=False).astype(jnp.bfloat16)
    return jnp.dot(activated, weight_out, preferred_element_type=jnp.float32).astype(jnp.bfloat16)

def reference(tokens, bottleneck, clip_ids, expert_ids, slots, norm1_gain, attn_qkv, attn_out, norm2_gain, router, fc_in, fc_out):
    model_width = tokens.shape[-1]
    blocks = tokens.shape[1] // TOK_DEV
    latent = bottleneck.reshape(blocks, CLIPS_DEV, NB, model_width)
    starts = jnp.arange(blocks, dtype=jnp.int32) * CLIPS_DEV
    block_of = jnp.arange(blocks * TOK_DEV, dtype=jnp.int32) // TOK_DEV
    column = jnp.arange(EXPERTS, dtype=jnp.int32)
    slot_total = EXPERTS * blocks * CAP
    outputs = []
    latents = []
    for modality in range(2):

        def one_block(operands):
            token_rows, latent_rows, token_clip, clip_start = operands
            return attend(token_rows, latent_rows, token_clip, clip_start, norm1_gain[modality], attn_qkv[modality], attn_out[modality])
        mid_tokens, mid_latent = lax.map(one_block, (tokens[modality].reshape(blocks, TOK_DEV, model_width), latent, clip_ids[modality].reshape(blocks, TOK_DEV), starts))
        mid_tokens = mid_tokens.reshape(blocks * TOK_DEV, model_width)
        latents.append(mid_latent)
        expert_in = layer_norm(mid_tokens, norm2_gain[modality]).astype(jnp.bfloat16)
        logits = jnp.dot(expert_in, router, preferred_element_type=jnp.float32)
        chosen = expert_ids[modality].astype(jnp.int32)
        slot_ids = slots[modality].astype(jnp.int32)
        picked = lax.optimization_barrier(jnp.sum(jnp.where(column[None, :] == chosen[:, None], logits, jnp.zeros_like(logits)), axis=1))
        gate_value = jax.nn.sigmoid(picked)
        served = slot_ids < CAP
        position = jnp.where(served, chosen * (blocks * CAP) + block_of * CAP + slot_ids, slot_total).astype(jnp.int32)
        buffer = jnp.zeros((slot_total, model_width), jnp.bfloat16).at[position].set(expert_in, mode='drop')
        served_rows = lax.map(expert_step, (buffer.reshape(EXPERTS, blocks * CAP, model_width), fc_in, fc_out))
        served_rows = served_rows.reshape(slot_total, model_width)
        returned = jnp.take(served_rows, position, axis=0, mode='fill', fill_value=0)
        outputs.append((mid_tokens + gate_value[:, None] * returned.astype(jnp.float32)).astype(jnp.bfloat16))
    mixed_tokens = jnp.stack(outputs)
    new_bottleneck = ((latents[0] + latents[1]) * 0.5).astype(jnp.bfloat16).reshape(blocks * CLIPS_DEV, NB, model_width)
    return (mixed_tokens, new_bottleneck)
```

```python
import functools
import math

import jax
import jax.numpy as jnp
from jax import lax
from jax.experimental import pallas as pl
from jax.experimental.pallas import tpu as pltpu
from jax.sharding import PartitionSpec as P

MESH = pl.DeviceIdType.MESH
HEAD = 64
CAP_FACTOR = 2


EPSILON = 1e-06


def layer_norm(features, scales):
    row_mean = jnp.mean(features, axis=-1, keepdims=True)
    centred = features - row_mean
    spread = jnp.mean(centred * centred, axis=-1, keepdims=True)
    return centred * lax.rsqrt(spread + EPSILON) * scales.astype(jnp.float32)


def attend(token_rows, latent_rows, token_clip, clip_start, scales, w_qkv, w_out):
    n_clips, n_latent, model_width = latent_rows.shape
    n_tokens = token_rows.shape[0]
    all_rows = jnp.concatenate(
        [token_rows, latent_rows.reshape(n_clips * n_latent, model_width)], axis=0
    )
    row_count = all_rows.shape[0]
    head_count = model_width // HEAD
    normed = layer_norm(all_rows.astype(jnp.float32), scales).astype(jnp.bfloat16)
    packed = jnp.dot(normed, w_qkv, preferred_element_type=jnp.float32).astype(jnp.bfloat16)
    queries = packed[:, :model_width].reshape(row_count, head_count, HEAD)
    key_rows = packed[:, model_width : 2 * model_width].reshape(row_count, head_count, HEAD)
    value_rows = packed[:, 2 * model_width :].reshape(row_count, head_count, HEAD)
    latent_clip = clip_start + jnp.arange(n_clips * n_latent, dtype=jnp.int32) // n_latent
    row_clip = jnp.concatenate([token_clip, latent_clip])
    allowed = row_clip[:, None] == row_clip[None, :]
    scores = jnp.einsum("qhd,khd->hqk", queries, key_rows, preferred_element_type=jnp.float32) * (
        1.0 / math.sqrt(HEAD)
    )
    scores = jnp.where(allowed[None, :, :], scores, -jnp.inf)
    row_max = jnp.max(scores, axis=-1, keepdims=True)
    weights = jnp.exp(scores - row_max)
    attn_weights = (weights / jnp.sum(weights, axis=-1, keepdims=True)).astype(jnp.bfloat16)
    attended = jnp.einsum(
        "hqk,khd->qhd", attn_weights, value_rows, preferred_element_type=jnp.float32
    )
    attended = attended.reshape(row_count, model_width).astype(jnp.bfloat16)
    updated = all_rows.astype(jnp.float32) + jnp.dot(
        attended, w_out, preferred_element_type=jnp.float32
    )
    return (updated[:n_tokens], updated[n_tokens:].reshape(n_clips, n_latent, model_width))


def gelu(x):
    half = 0.5 * x
    return half + half * lax.erf(x * (1.0 / math.sqrt(2.0)))


def near_count(size):
    return 4 if size % 4 == 0 else 1


def moe_kernel(
    size,
    cap,
    tile,
    latent_ref,
    buf_ref,
    w_in_hbm,
    w_out_hbm,
    out_ref,
    mean_ref,
    w_in,
    w_out,
    recv,
    res,
    acc,
    act,
    peer_latent,
    w_sems,
    own_sems,
    lat_sems,
    send_sems,
    recv_sems,
    back_send,
    back_recv,
):
    near = near_count(size)
    far = size // near
    me = lax.axis_index("exp")
    mod = lax.axis_index("mod")
    high, low = me // near, me % near
    shifts = [0] + sorted(range(1, far), key=lambda s: (abs(2 * s - far), s))
    order = [(s, d) for s in shifts for d in range(near)]

    def ahead(step):
        s, d = order[step]
        return ((high + s) % far) * near + (low + d) % near

    def behind(step):
        s, d = order[step]
        return ((high + far - s) % far) * near + (low + near - d) % near

    def block(index):
        return pl.ds(pl.multiple_of(index * cap, cap), cap)

    load_in = pltpu.make_async_copy(w_in_hbm, w_in, w_sems.at[0])
    load_out = pltpu.make_async_copy(w_out_hbm, w_out, w_sems.at[1])
    load_in.start()
    load_out.start()

    barrier = pltpu.get_barrier_semaphore()
    for step in range(1, size):
        pl.semaphore_signal(barrier, inc=1, device_id=(mod, ahead(step)), device_id_type=MESH)
    pl.semaphore_signal(barrier, inc=1, device_id=(1 - mod, me), device_id_type=MESH)
    pl.semaphore_wait(barrier, size)

    sends = [None]
    for step in range(1, size):
        sends.append(
            pltpu.make_async_remote_copy(
                src_ref=buf_ref.at[block(ahead(step))],
                dst_ref=recv.at[pl.ds(step * cap, cap)],
                send_sem=send_sems.at[step],
                recv_sem=recv_sems.at[step],
                device_id=(mod, ahead(step)),
                device_id_type=MESH,
            )
        )
    backs = [None]
    for step in range(1, size):
        backs.append(
            pltpu.make_async_remote_copy(
                src_ref=res.at[pl.ds(step * cap, cap)],
                dst_ref=out_ref.at[block(me)],
                send_sem=back_send.at[step],
                recv_sem=back_recv.at[step],
                device_id=(mod, behind(step)),
                device_id_type=MESH,
            )
        )
    for step in range(1, size):
        sends[step].start()
    latent_copy = pltpu.make_async_remote_copy(
        src_ref=latent_ref,
        dst_ref=peer_latent,
        send_sem=lat_sems.at[0],
        recv_sem=lat_sems.at[1],
        device_id=(1 - mod, me),
        device_id_type=MESH,
    )
    latent_copy.start()
    own = pltpu.make_async_copy(buf_ref.at[block(me)], recv.at[pl.ds(0, cap)], own_sems.at[0])
    own.start()
    own.wait()

    groups = 4 if size % 4 == 0 else 1
    per = size // groups
    rows = per * cap
    tiles = w_in.shape[1] // tile
    own_back = pltpu.make_async_copy(res.at[pl.ds(0, cap)], out_ref.at[block(me)], own_sems.at[1])
    for g in range(groups):
        for step in range(g * per, (g + 1) * per):
            if step:
                sends[step].wait_recv()
        if g == 0:
            load_in.wait()
            load_out.wait()
        here = pl.ds(g * rows, rows)

        def hidden(t):
            cols = pl.ds(pl.multiple_of(t * tile, tile), tile)
            return gelu(
                jnp.dot(recv[here, :], w_in[:, cols], preferred_element_type=jnp.float32)
            ).astype(jnp.bfloat16)

        def project(t, slot):
            cols = pl.ds(pl.multiple_of(t * tile, tile), tile)
            return jnp.dot(act[slot], w_out[cols, :], preferred_element_type=jnp.float32)

        act[0] = hidden(0)
        acc[...] = jnp.zeros_like(acc)

        def body(t, carry):
            acc[...] += project(t - 1, (t + 1) % 2)
            act[t % 2] = hidden(t)
            return carry

        lax.fori_loop(1, tiles, body, 0)
        res[here, :] = (acc[...] + project(tiles - 1, (tiles - 1) % 2)).astype(jnp.bfloat16)
        for step in range(g * per, (g + 1) * per):
            if step:
                backs[step].start()
            else:
                own_back.start()

    latent_copy.wait()
    mean_ref[...] = ((latent_ref[...] + peer_latent[...]) * 0.5).astype(jnp.bfloat16)
    own_back.wait()
    for step in range(1, size):
        sends[step].wait_send()
        backs[step].wait()


def exchange_experts(mid_latent, buffer, weight_in, weight_out, size):
    rows, width = buffer.shape
    cap = rows // size
    hidden_width = weight_in.shape[1]
    tile = 512
    groups = 4 if size % 4 == 0 else 1
    vmem = pl.BlockSpec(memory_space=pltpu.VMEM)
    hbm = pl.BlockSpec(memory_space=pl.ANY)
    return pl.pallas_call(
        functools.partial(moe_kernel, size, cap, tile),
        out_shape=(
            jax.ShapeDtypeStruct((rows, width), jnp.bfloat16),
            jax.ShapeDtypeStruct(mid_latent.shape, jnp.bfloat16),
        ),
        in_specs=[vmem, vmem, hbm, hbm],
        out_specs=(vmem, vmem),
        scratch_shapes=[
            pltpu.VMEM((width, hidden_width), jnp.bfloat16),
            pltpu.VMEM((hidden_width, width), jnp.bfloat16),
            pltpu.VMEM((rows, width), jnp.bfloat16),
            pltpu.VMEM((rows, width), jnp.bfloat16),
            pltpu.VMEM((rows // groups, width), jnp.float32),
            pltpu.VMEM((2, rows // groups, tile), jnp.bfloat16),
            pltpu.VMEM(mid_latent.shape, jnp.float32),
            pltpu.SemaphoreType.DMA((2,)),
            pltpu.SemaphoreType.DMA((2,)),
            pltpu.SemaphoreType.DMA((2,)),
            pltpu.SemaphoreType.DMA((size,)),
            pltpu.SemaphoreType.DMA((size,)),
            pltpu.SemaphoreType.DMA((size,)),
            pltpu.SemaphoreType.DMA((size,)),
        ],
        compiler_params=pltpu.CompilerParams(
            collective_id=0, has_side_effects=True, vmem_limit_bytes=48 * 1024 * 1024
        ),
    )(mid_latent, buffer, weight_in, weight_out)


def mixture(mid_tokens, mid_latent, chosen, slot_ids, scales, router, fc_in, fc_out):
    model_width = mid_tokens.shape[1]
    expert_count = router.shape[1]
    capacity = CAP_FACTOR * mid_tokens.shape[0] // expert_count
    slot_total = expert_count * capacity
    expert_in = layer_norm(mid_tokens, scales).astype(jnp.bfloat16)
    logits = jnp.dot(expert_in, router, preferred_element_type=jnp.float32)
    column = jnp.arange(expert_count, dtype=jnp.int32)
    picked = jnp.sum(
        jnp.where(column[None, :] == chosen[:, None], logits, jnp.zeros_like(logits)), axis=1
    )
    gate_value = jax.nn.sigmoid(picked)
    served = slot_ids < capacity
    position = jnp.where(served, chosen * capacity + slot_ids, slot_total)
    places = jnp.arange(slot_total, dtype=jnp.int32)
    to_slot = (places[:, None] == position[None, :]).astype(jnp.bfloat16)
    buffer = jnp.dot(to_slot, expert_in, preferred_element_type=jnp.float32).astype(jnp.bfloat16)
    results, new_bottleneck = exchange_experts(
        mid_latent.reshape(-1, model_width), buffer, fc_in[0], fc_out[0], expert_count
    )
    from_slot = (position[:, None] == places[None, :]).astype(jnp.bfloat16)
    returned = jnp.dot(from_slot, results, preferred_element_type=jnp.float32)
    mixed = (mid_tokens + gate_value[:, None] * returned).astype(jnp.bfloat16)
    return mixed, new_bottleneck.reshape(mid_latent.shape)


def on_device(
    tokens,
    bottleneck,
    clip_ids,
    expert_ids,
    slots,
    norm1_gain,
    attn_qkv,
    attn_out,
    norm2_gain,
    router,
    fc_in,
    fc_out,
):
    clip_start = lax.axis_index("exp") * bottleneck.shape[0]
    mid_tokens, mid_latent = attend(
        tokens[0], bottleneck, clip_ids[0], clip_start, norm1_gain[0], attn_qkv[0], attn_out[0]
    )
    mixed_tokens, new_bottleneck = mixture(
        mid_tokens, mid_latent, expert_ids[0], slots[0], norm2_gain[0], router, fc_in, fc_out
    )
    return (mixed_tokens[None], new_bottleneck)


def solution(mesh):
    in_specs = (
        P("mod", "exp", None),
        P("exp", None, None),
        P("mod", "exp"),
        P("mod", "exp"),
        P("mod", "exp"),
        P("mod", None),
        P("mod", None, None),
        P("mod", None, None),
        P("mod", None),
        P(),
        P("exp", None, None),
        P("exp", None, None),
    )
    out_specs = (P("mod", "exp", None), P("exp", None, None))
    return jax.shard_map(
        on_device, mesh=mesh, in_specs=in_specs, out_specs=out_specs, check_vma=False
    )
```

```python
import functools
import math

import jax
import jax.numpy as jnp
from jax import lax
from jax.experimental import pallas as pl
from jax.experimental.pallas import tpu as pltpu
from jax.sharding import PartitionSpec as P

MESH = pl.DeviceIdType.MESH
HEAD = 64
CAP_FACTOR = 2


EPSILON = 1e-06


def layer_norm(features, scales):
    row_mean = jnp.mean(features, axis=-1, keepdims=True)
    centred = features - row_mean
    spread = jnp.mean(centred * centred, axis=-1, keepdims=True)
    return centred * lax.rsqrt(spread + EPSILON) * scales.astype(jnp.float32)


def attention_kernel(pair, rows_ref, cols_ref, q_ref, k_ref, v_ref, out_ref):
    allowed = rows_ref[...] == cols_ref[...]
    lane = lax.broadcasted_iota(jnp.int32, q_ref.shape, 1) // HEAD
    queries = q_ref[...] * jnp.bfloat16(1.0 / math.sqrt(HEAD))
    attended = jnp.zeros(out_ref.shape, jnp.float32)
    for head in range(pair):
        mine = lane == head
        scores = lax.dot_general(
            jnp.where(mine, queries, jnp.zeros_like(queries)),
            k_ref[...],
            (((1,), (1,)), ((), ())),
            preferred_element_type=jnp.float32,
        )
        scores = jnp.where(allowed, scores, -jnp.inf)
        weights = jnp.exp(scores - jnp.max(scores, axis=-1, keepdims=True))
        total = jnp.sum(weights, axis=-1, keepdims=True)
        summed = jnp.dot(
            weights.astype(jnp.bfloat16), v_ref[...], preferred_element_type=jnp.float32
        )
        attended = jnp.where(mine, summed / total, attended)
    out_ref[...] = attended.astype(jnp.bfloat16)


def attention(packed, row_clip):
    rows, width = packed.shape[0], packed.shape[1] // 3
    pair = 128 // HEAD
    steps = width // 128

    def part(index):
        return pl.BlockSpec((rows, 128), lambda step: (0, index * steps + step))

    return pl.pallas_call(
        functools.partial(attention_kernel, pair),
        grid=(steps,),
        out_shape=jax.ShapeDtypeStruct((rows, width), jnp.bfloat16),
        in_specs=[
            pl.BlockSpec((rows, 1), lambda step: (0, 0)),
            pl.BlockSpec((1, rows), lambda step: (0, 0)),
            part(0),
            part(1),
            part(2),
        ],
        out_specs=pl.BlockSpec((rows, 128), lambda step: (0, step)),
        compiler_params=pltpu.CompilerParams(vmem_limit_bytes=32 * 1024 * 1024),
    )(row_clip[:, None], row_clip[None, :], packed, packed, packed)


def attend(token_rows, latent_rows, token_clip, clip_start, scales, w_qkv, w_out):
    n_clips, n_latent, model_width = latent_rows.shape
    n_tokens = token_rows.shape[0]
    all_rows = jnp.concatenate(
        [token_rows, latent_rows.reshape(n_clips * n_latent, model_width)], axis=0
    )
    row_count = all_rows.shape[0]
    normed = layer_norm(all_rows.astype(jnp.float32), scales).astype(jnp.bfloat16)
    packed = jnp.dot(normed, w_qkv, preferred_element_type=jnp.float32).astype(jnp.bfloat16)
    latent_clip = clip_start + jnp.arange(n_clips * n_latent, dtype=jnp.int32) // n_latent
    row_clip = jnp.concatenate([token_clip, latent_clip])
    attended = attention(packed, row_clip)
    updated = all_rows.astype(jnp.float32) + jnp.dot(
        attended, w_out, preferred_element_type=jnp.float32
    )
    return (updated[:n_tokens], updated[n_tokens:].reshape(n_clips, n_latent, model_width))


def gelu(x):
    half = 0.5 * x
    return half + half * lax.erf(x * (1.0 / math.sqrt(2.0)))


def near_count(size):
    return 4 if size % 4 == 0 else 1


def moe_kernel(
    size,
    cap,
    tile,
    latent_ref,
    buf_ref,
    w_in_hbm,
    w_out_hbm,
    out_ref,
    mean_ref,
    w_in,
    w_out,
    recv,
    res,
    acc,
    act,
    peer_latent,
    w_sems,
    own_sems,
    lat_sems,
    send_sems,
    recv_sems,
    back_send,
    back_recv,
):
    near = near_count(size)
    far = size // near
    me = lax.axis_index("exp")
    mod = lax.axis_index("mod")
    high, low = me // near, me % near
    shifts = [0] + sorted(range(1, far), key=lambda s: (abs(2 * s - far), s))
    order = [(s, d) for s in shifts for d in range(near)]

    def ahead(step):
        s, d = order[step]
        return ((high + s) % far) * near + (low + d) % near

    def behind(step):
        s, d = order[step]
        return ((high + far - s) % far) * near + (low + near - d) % near

    def block(index):
        return pl.ds(pl.multiple_of(index * cap, cap), cap)

    load_in = pltpu.make_async_copy(w_in_hbm, w_in, w_sems.at[0])
    load_out = pltpu.make_async_copy(w_out_hbm, w_out, w_sems.at[1])
    load_in.start()
    load_out.start()

    barrier = pltpu.get_barrier_semaphore()
    for step in range(1, size):
        pl.semaphore_signal(barrier, inc=1, device_id=(mod, ahead(step)), device_id_type=MESH)
    pl.semaphore_signal(barrier, inc=1, device_id=(1 - mod, me), device_id_type=MESH)
    pl.semaphore_wait(barrier, size)

    sends = [None]
    for step in range(1, size):
        sends.append(
            pltpu.make_async_remote_copy(
                src_ref=buf_ref.at[block(ahead(step))],
                dst_ref=recv.at[pl.ds(step * cap, cap)],
                send_sem=send_sems.at[step],
                recv_sem=recv_sems.at[step],
                device_id=(mod, ahead(step)),
                device_id_type=MESH,
            )
        )
    backs = [None]
    for step in range(1, size):
        backs.append(
            pltpu.make_async_remote_copy(
                src_ref=res.at[pl.ds(step * cap, cap)],
                dst_ref=out_ref.at[block(me)],
                send_sem=back_send.at[step],
                recv_sem=back_recv.at[step],
                device_id=(mod, behind(step)),
                device_id_type=MESH,
            )
        )
    for step in range(1, size):
        sends[step].start()
    latent_copy = pltpu.make_async_remote_copy(
        src_ref=latent_ref,
        dst_ref=peer_latent,
        send_sem=lat_sems.at[0],
        recv_sem=lat_sems.at[1],
        device_id=(1 - mod, me),
        device_id_type=MESH,
    )
    latent_copy.start()
    own = pltpu.make_async_copy(buf_ref.at[block(me)], recv.at[pl.ds(0, cap)], own_sems.at[0])
    own.start()
    own.wait()

    groups = 2 if size % 4 == 0 else 1
    per = size // groups
    rows = per * cap
    tiles = w_in.shape[1] // tile
    own_back = pltpu.make_async_copy(res.at[pl.ds(0, cap)], out_ref.at[block(me)], own_sems.at[1])
    for g in range(groups):
        for step in range(g * per, (g + 1) * per):
            if step:
                sends[step].wait_recv()
        if g == 0:
            load_in.wait()
            load_out.wait()
        here = pl.ds(g * rows, rows)

        def hidden(t):
            cols = pl.ds(pl.multiple_of(t * tile, tile), tile)
            return gelu(
                jnp.dot(recv[here, :], w_in[:, cols], preferred_element_type=jnp.float32)
            ).astype(jnp.bfloat16)

        def project(t, slot):
            cols = pl.ds(pl.multiple_of(t * tile, tile), tile)
            return jnp.dot(act[slot], w_out[cols, :], preferred_element_type=jnp.float32)

        act[0] = hidden(0)
        acc[...] = jnp.zeros_like(acc)

        def body(t, carry):
            acc[...] += project(t - 1, (t + 1) % 2)
            act[t % 2] = hidden(t)
            return carry

        lax.fori_loop(1, tiles, body, 0)
        res[here, :] = (acc[...] + project(tiles - 1, (tiles - 1) % 2)).astype(jnp.bfloat16)
        for step in range(g * per, (g + 1) * per):
            if step:
                backs[step].start()
            else:
                own_back.start()

    latent_copy.wait()
    mean_ref[...] = ((latent_ref[...] + peer_latent[...]) * 0.5).astype(jnp.bfloat16)
    own_back.wait()
    for step in range(1, size):
        sends[step].wait_send()
        backs[step].wait()


def exchange_experts(mid_latent, buffer, weight_in, weight_out, size):
    rows, width = buffer.shape
    cap = rows // size
    hidden_width = weight_in.shape[1]
    tile = 1024
    groups = 2 if size % 4 == 0 else 1
    vmem = pl.BlockSpec(memory_space=pltpu.VMEM)
    hbm = pl.BlockSpec(memory_space=pl.ANY)
    return pl.pallas_call(
        functools.partial(moe_kernel, size, cap, tile),
        out_shape=(
            jax.ShapeDtypeStruct((rows, width), jnp.bfloat16),
            jax.ShapeDtypeStruct(mid_latent.shape, jnp.bfloat16),
        ),
        in_specs=[vmem, vmem, hbm, hbm],
        out_specs=(vmem, vmem),
        scratch_shapes=[
            pltpu.VMEM((width, hidden_width), jnp.bfloat16),
            pltpu.VMEM((hidden_width, width), jnp.bfloat16),
            pltpu.VMEM((rows, width), jnp.bfloat16),
            pltpu.VMEM((rows, width), jnp.bfloat16),
            pltpu.VMEM((rows // groups, width), jnp.float32),
            pltpu.VMEM((2, rows // groups, tile), jnp.bfloat16),
            pltpu.VMEM(mid_latent.shape, jnp.float32),
            pltpu.SemaphoreType.DMA((2,)),
            pltpu.SemaphoreType.DMA((2,)),
            pltpu.SemaphoreType.DMA((2,)),
            pltpu.SemaphoreType.DMA((size,)),
            pltpu.SemaphoreType.DMA((size,)),
            pltpu.SemaphoreType.DMA((size,)),
            pltpu.SemaphoreType.DMA((size,)),
        ],
        compiler_params=pltpu.CompilerParams(
            collective_id=0, has_side_effects=True, vmem_limit_bytes=48 * 1024 * 1024
        ),
    )(mid_latent, buffer, weight_in, weight_out)


def mixture(mid_tokens, mid_latent, chosen, slot_ids, scales, router, fc_in, fc_out):
    model_width = mid_tokens.shape[1]
    expert_count = router.shape[1]
    capacity = CAP_FACTOR * mid_tokens.shape[0] // expert_count
    slot_total = expert_count * capacity
    expert_in = layer_norm(mid_tokens, scales).astype(jnp.bfloat16)
    logits = jnp.dot(expert_in, router, preferred_element_type=jnp.float32)
    column = jnp.arange(expert_count, dtype=jnp.int32)
    picked = jnp.sum(
        jnp.where(column[None, :] == chosen[:, None], logits, jnp.zeros_like(logits)), axis=1
    )
    gate_value = jax.nn.sigmoid(picked)
    served = slot_ids < capacity
    position = jnp.where(served, chosen * capacity + slot_ids, slot_total)
    places = jnp.arange(slot_total, dtype=jnp.int32)
    to_slot = (places[:, None] == position[None, :]).astype(jnp.bfloat16)
    buffer = jnp.dot(to_slot, expert_in, preferred_element_type=jnp.float32).astype(jnp.bfloat16)
    results, new_bottleneck = exchange_experts(
        mid_latent.reshape(-1, model_width), buffer, fc_in[0], fc_out[0], expert_count
    )
    from_slot = (position[:, None] == places[None, :]).astype(jnp.bfloat16)
    returned = jnp.dot(from_slot, results, preferred_element_type=jnp.float32)
    mixed = (mid_tokens + gate_value[:, None] * returned).astype(jnp.bfloat16)
    return mixed, new_bottleneck.reshape(mid_latent.shape)


def on_device(
    tokens,
    bottleneck,
    clip_ids,
    expert_ids,
    slots,
    norm1_gain,
    attn_qkv,
    attn_out,
    norm2_gain,
    router,
    fc_in,
    fc_out,
):
    clip_start = lax.axis_index("exp") * bottleneck.shape[0]
    mid_tokens, mid_latent = attend(
        tokens[0], bottleneck, clip_ids[0], clip_start, norm1_gain[0], attn_qkv[0], attn_out[0]
    )
    mixed_tokens, new_bottleneck = mixture(
        mid_tokens, mid_latent, expert_ids[0], slots[0], norm2_gain[0], router, fc_in, fc_out
    )
    return (mixed_tokens[None], new_bottleneck)


def solution(mesh):
    in_specs = (
        P("mod", "exp", None),
        P("exp", None, None),
        P("mod", "exp"),
        P("mod", "exp"),
        P("mod", "exp"),
        P("mod", None),
        P("mod", None, None),
        P("mod", None, None),
        P("mod", None),
        P(),
        P("exp", None, None),
        P("exp", None, None),
    )
    out_specs = (P("mod", "exp", None), P("exp", None, None))
    return jax.shard_map(
        on_device, mesh=mesh, in_specs=in_specs, out_specs=out_specs, check_vma=False
    )
```
